32 devices in a mesh: rows: 8 (over z, x), cols: 4 (over y, core).
Axes of the slice: x: 2, y: 2, z: 4, core: 2. Of those that a mesh axis runs over, the one named last changes fastest.
Arguments:
- panel: float32 [4096, 1024], P('rows'), as said below
- window_block: float32 [4096, 2048], P('rows', 'cols'), may hold values from -6 to 6
- row_live: int32 [8], replicated, may hold values 0 or 1
- window_rows: int32 [4], replicated, may hold values from 2 to 7, as said below
Outputs:
- factor: float32 [4096, 1024], P('rows')
- updated: float32 [4096, 2048], P('rows', 'cols')
The draws below stay inside these ranges and needn't reach their ends.
Inputs may be any that keep to these rules, and one draw needn't show every extreme that they name: `window_rows`: distinct tile rows, none inside the supernode. `row_live`: the value for tile rows below 2 is ignored: those rows are always present. `panel`: the first 1024 rows hold a symmetric positive definite block.
All inputs are finite; a program needn't handle non-finite values.
Results may differ from the reference program's by a relative error of at most 0.0001.
Values sent between devices are 32-bit elements; how exact they have to be, the bound alone decides.
A program may use at most 128 MiB of HBM per device.

```python
import jax
import jax.numpy as jnp
from jax import lax

B = 512
P_SIZE = 2
NT = 8
NW = 4


def draw_window_rows(key, part):
    pair = jax.random.split(key, 2)
    first = jax.random.randint(pair[0], (NT - P_SIZE,), 0, 1 << 14)
    second = jax.random.randint(pair[1], (NT - P_SIZE,), 0, 1 << 14)
    scores = (first * 16384 + second) % 1048576
    distinct = scores * NT + jnp.arange(NT - P_SIZE)
    values, places = lax.top_k(distinct, NW)
    return (places + P_SIZE).astype(jnp.int32)


def draw_panel(key, part):
    keys = jax.random.split(jax.random.fold_in(key, 5), 5)
    total_rows = NT * B
    width = P_SIZE * B
    reach = max(4.0, width / 48.0)
    base = jax.random.normal(keys[0], (total_rows, width)) * 0.25
    rough = jax.random.normal(keys[1], (width, width)) * (0.15 / width ** 0.5)
    rough = (rough + rough.T) * 0.70710678
    places = jnp.arange(width).astype(jnp.float32)
    distance = jnp.abs(places[:, None] - places[None, :])
    kernel = 0.6 * jnp.exp(-distance / reach)
    diag_vals = jax.random.uniform(keys[2], (width,), minval=0.8, maxval=1.6)
    scales = jnp.exp(jax.random.uniform(keys[4], (width,), minval=jnp.log(0.8), maxval=jnp.log(1.25)))
    head = scales[:, None] * scales[None, :] * (kernel + rough) + jnp.diag(diag_vals)
    head_full = jnp.concatenate([head, jnp.zeros((total_rows - width, width), jnp.float32)], axis=0)
    row_ids = jnp.arange(total_rows)[:, None]
    return jnp.where(row_ids < width, head_full, base).astype(jnp.float32)


def set_ends(array, stream_key, smallest, largest):
    extent = array.shape
    place = [jax.random.randint(jax.random.fold_in(stream_key, axis), (), 0, extent[axis]) for axis in range(len(extent))]
    array = array.at[tuple(place)].set(smallest)
    longest = extent.index(max(extent))
    place[longest] = (place[longest] + 1) % extent[longest]
    return array.at[tuple(place)].set(largest)


def block_levels(rng, shape, pieces, low, largest):
    loudness, own = 1.0, jax.random.fold_in(rng, 6)
    for position, blocks in pieces:
        draws = jnp.exp(jax.random.uniform(jax.random.fold_in(own, position), (blocks,), jnp.float32, low / len(pieces), largest / len(pieces)))
        loudness = loudness * jnp.repeat(draws, shape[position] // blocks).reshape([-1 if axis == position else 1 for axis in range(len(shape))])
    return loudness


def noise(rng, extent, spread, most, cuts=(), dtype=jnp.bfloat16):
    result = spread * jax.random.normal(rng, extent, jnp.float32)
    if cuts:
        result = result * block_levels(rng, extent, cuts, -0.22, 0.18)
    return jnp.clip(result, -most, most).astype(dtype)


def setup_inputs(seed: int = 0) -> dict:
    arg_keys = jax.random.split(jax.random.key(seed), 5)
    return {
        "panel": draw_panel(jax.random.fold_in(arg_keys[4], 71), 0),
        "window_block": noise(arg_keys[1], (NT * B, NW * B), 1.0, 6.0, ((0, 8), (1, 4)), jnp.float32),
        "row_live": set_ends((jax.random.randint(arg_keys[2], (NT,), 0, 4) < 3).astype(jnp.int32), jax.random.fold_in(arg_keys[2], 1), 0, 1),
        "window_rows": draw_window_rows(jax.random.fold_in(arg_keys[4], 71), 0),
    }


def reference(panel, window_block, row_live, window_rows):
    tile_ids = jnp.arange(NT)
    live_flag = jnp.where(tile_ids < P_SIZE, 1, row_live).astype(jnp.float32)
    scaled = panel * jnp.repeat(live_flag, B)[:, None]
    head = scaled[:P_SIZE * B]
    square = jnp.tril(head) + jnp.tril(head, -1).T
    lower = jnp.linalg.cholesky(square)
    solved = lax.linalg.triangular_solve(lower, scaled, left_side=False, lower=True, transpose_a=True)
    factor = jnp.concatenate([lower, solved[P_SIZE * B:]], axis=0)
    columns = []
    for window in range(NW):
        start = (window_rows[window] * B).astype(jnp.int32)
        target_row = lax.dynamic_slice_in_dim(factor, start, B, 0)
        block_now = window_block[:, window * B:(window + 1) * B]
        product = lax.dot_general(factor, target_row, (((1,), (1,)), ((), ())), precision=lax.Precision.HIGHEST)
        columns.append(block_now - product)
    return (factor, jnp.concatenate(columns, axis=1))
```

```python
import functools

import jax
import jax.numpy as jnp
from jax import lax
from jax.experimental import pallas as pl
from jax.experimental.pallas import tpu as pltpu
from jax.sharding import PartitionSpec as P

P_SIZE = 2
HIGHEST = lax.Precision.HIGHEST
CONTRACT = (((1,), (1,)), ((), ()))
LEAF = 128
GROUP = 8
WIDE = 256
MESH = pl.DeviceIdType.MESH


def times_trans(left, right):
    return lax.dot_general(left, right, CONTRACT, precision=HIGHEST, preferred_element_type=jnp.float32)


def spread_kernel(n_rows, n_cols, panel, first, second, row_send, row_recv, col_send, col_recv):
    r = lax.axis_index("rows")
    c = lax.axis_index("cols")
    width = panel.shape[0]
    share = width // n_cols
    pieces = []
    for half in range(2):
        pieces.append((0, half * (share // 2), share // 2))
    for quarter in range(4):
        pieces.append((1, quarter * (share // 4), share // 4))

    barrier = pltpu.get_barrier_semaphore()
    for step in range(1, n_cols):
        other = lax.rem(c + step, n_cols)
        pl.semaphore_signal(barrier, inc=1, device_id=(r, other), device_id_type=MESH)

    @pl.when(r < 2)
    def _():
        pl.semaphore_signal(barrier, inc=1, device_id=(1 - r, c), device_id_type=MESH)

    @pl.when(r >= 2)
    def _():
        pl.semaphore_signal(barrier, inc=1, device_id=(r - 2, c), device_id_type=MESH)

    @pl.when(r + 2 < n_rows)
    def _():
        pl.semaphore_signal(barrier, inc=1, device_id=(r + 2, c), device_id_type=MESH)

    pl.semaphore_wait(barrier, n_cols + (r + 2 < n_rows).astype(jnp.int32))

    def window(ref, piece, owner):
        which, start, size = pieces[piece]
        return ref.at[pl.ds(pl.multiple_of(owner * share + start, 8), size), :]

    def to_row(piece, slot, dest, own):
        which, start, size = pieces[piece]
        dst = window((first, second)[which], piece, c)
        if own:
            src = panel.at[pl.ds(pl.multiple_of(c * share + start, 8), size), pl.ds(0, dst.shape[1])]
        else:
            src = dst
        return pltpu.make_async_remote_copy(
            src_ref=src, dst_ref=dst, send_sem=row_send.at[piece, slot], recv_sem=row_recv.at[piece],
            device_id=(dest, c), device_id_type=MESH)

    def to_col(piece, step):
        ref = (first, second)[pieces[piece][0]]
        return pltpu.make_async_remote_copy(
            src_ref=window(ref, piece, c), dst_ref=window(ref, piece, c),
            send_sem=col_send.at[piece, step - 1], recv_sem=col_recv.at[piece, step - 1],
            device_id=(r, lax.rem(c + step, n_cols)), device_id_type=MESH)

    for piece in range(len(pieces)):
        which = pieces[piece][0]

        @pl.when(r == which)
        def _():
            to_row(piece, 0, 1 - which, True).start()
            if which + 2 < n_rows:
                to_row(piece, 1, which + 2, True).start()

    @pl.when(r == 0)
    def _():
        first[...] = panel[:, : first.shape[1]]

    @pl.when(r == 1)
    def _():
        second[...] = panel[...]

    for piece in range(len(pieces)):
        which = pieces[piece][0]

        @pl.when(r != which)
        def _():
            to_row(piece, 0, r, False).wait_recv()

            @pl.when(r + 2 < n_rows)
            def _():
                to_row(piece, 0, r + 2, False).start()

            for step in range(1, n_cols):
                to_col(piece, step).start()

    for piece in range(len(pieces)):
        which = pieces[piece][0]

        @pl.when(r != which)
        def _():
            for step in range(1, n_cols):
                to_col(piece, step).wait_recv()
            for step in range(1, n_cols):
                to_col(piece, step).wait_send()

            @pl.when(r + 2 < n_rows)
            def _():
                to_row(piece, 0, r + 2, False).wait_send()

        @pl.when(r == which)
        def _():
            to_row(piece, 0, 1 - which, True).wait_send()
            if which + 2 < n_rows:
                to_row(piece, 1, which + 2, True).wait_send()


def spread(panel, n_rows, n_cols):
    width = panel.shape[0]
    n_pieces = 6
    return pl.pallas_call(
        functools.partial(spread_kernel, n_rows, n_cols),
        out_shape=(
            jax.ShapeDtypeStruct((width, width), jnp.float32),
            jax.ShapeDtypeStruct((width, P_SIZE * width), jnp.float32),
        ),
        in_specs=[pl.BlockSpec(memory_space=pltpu.VMEM)],
        out_specs=(pl.BlockSpec(memory_space=pltpu.VMEM),) * 2,
        scratch_shapes=[
            pltpu.SemaphoreType.DMA((n_pieces, 2)),
            pltpu.SemaphoreType.DMA((n_pieces,)),
            pltpu.SemaphoreType.DMA((n_pieces, n_cols - 1)),
            pltpu.SemaphoreType.DMA((n_pieces, n_cols - 1)),
        ],
        compiler_params=pltpu.CompilerParams(
            collective_id=0, has_side_effects=True, vmem_limit_bytes=24 << 20),
        name="spread",
    )(panel)


def split3(value):
    high = value.astype(jnp.bfloat16).astype(jnp.float32)
    rest = value - high
    mid = rest.astype(jnp.bfloat16).astype(jnp.float32)
    return high, mid, rest - mid


def factor_leaf(aug, upper, inverse):
    lanes = lax.broadcasted_iota(jnp.int32, (GROUP, LEAF), 1)
    subs = lax.broadcasted_iota(jnp.int32, (GROUP, LEAF), 0)
    for g in range(LEAF // GROUP):
        base = g * GROUP
        left = aug[base : base + GROUP, :LEAF]
        right = aug[base : base + GROUP, LEAF:]
        cols = [
            jnp.broadcast_to(left[:, base + j : base + j + 1], (GROUP, LEAF)) for j in range(GROUP)
        ]
        scale = jnp.zeros((GROUP, LEAF), jnp.float32)
        for k in range(GROUP):
            pivot = jnp.broadcast_to(cols[k][k : k + 1, :], (GROUP, LEAF))
            root = lax.rsqrt(pivot)
            scale = jnp.where(subs == k, root, scale)
            if k + 1 < GROUP:
                mult = jnp.where(subs > k, cols[k] * (root * root), 0.0)
                for j in range(k + 1, GROUP):
                    cols[j] = cols[j] - mult * jnp.broadcast_to(cols[j][k : k + 1, :], (GROUP, LEAF))
                left = left - mult * jnp.broadcast_to(left[k : k + 1, :], (GROUP, LEAF))
                right = right - mult * jnp.broadcast_to(right[k : k + 1, :], (GROUP, LEAF))
        row_of = lanes - base
        left = jnp.where(row_of >= subs, left * scale, 0.0)
        right = right * scale
        upper[base : base + GROUP, :] = left
        inverse[base : base + GROUP, :] = right
        if base + GROUP < LEAF:
            lh, lm, ll = split3(left)
            rh, rm, rl = split3(right)
            keep = lanes >= base + GROUP
            a = [jnp.where(keep, v, 0.0) for v in (lh, lm, ll)]
            lhs = jnp.concatenate([a[0], a[0], a[1], a[0], a[1], a[2]], axis=0)
            rl_ = jnp.concatenate([lh, lm, lh, ll, lm, lh], axis=0)
            rr_ = jnp.concatenate([rh, rm, rh, rl, rm, rh], axis=0)
            rhs = jnp.concatenate([rl_, rr_], axis=1)
            update = lax.dot_general(
                lhs, rhs, (((0,), (0,)), ((), ())), preferred_element_type=jnp.float32)
            aug[base + GROUP :, :] = aug[base + GROUP :, :] - update[base + GROUP :, :]


def factor_kernel(first, second, lower, inverses, aug, upper, leaf_inv):
    width = first.shape[0]
    total = lower.shape[0]
    n_leaf = total // LEAF
    per = width // LEAF
    rows = lax.broadcasted_iota(jnp.int32, (LEAF, LEAF), 0)
    lanes = lax.broadcasted_iota(jnp.int32, (LEAF, LEAF), 1)
    lower[:width, :width] = first[...]
    lower[:width, width:] = jnp.zeros((width, total - width), jnp.float32)
    lower[width:, :] = second[...]
    for b in range(n_leaf - 1):
        lower[b * LEAF : (b + 1) * LEAF, (b + 1) * LEAF :] = jnp.zeros(
            (LEAF, total - (b + 1) * LEAF), jnp.float32)
    inverses[...] = jnp.zeros(inverses.shape, jnp.float32)

    def step(k, carry):
        at = pl.ds(pl.multiple_of(k * LEAF, LEAF), LEAF)
        block = lower[at, at]
        aug[:, :LEAF] = jnp.where(rows >= lanes, block, block.T)
        aug[:, LEAF:] = jnp.where(rows == lanes, 1.0, 0.0)
        factor_leaf(aug, upper, leaf_inv)
        lower[at, at] = upper[...].T
        for b in range(n_leaf):

            @pl.when(k == b)
            def _():
                lo, hi = b * LEAF, (b + 1) * LEAF
                wide = b * LEAF // WIDE
                off = lo - wide * WIDE
                inv = leaf_inv[...]
                inverses[wide, off : off + LEAF, off : off + LEAF] = inv
                if off:
                    before = inverses[wide, :LEAF, :LEAF]
                    cross = lower[lo:hi, lo - LEAF : lo]
                    part = lax.dot_general(
                        cross, before, (((1,), (0,)), ((), ())), precision=HIGHEST,
                        preferred_element_type=jnp.float32)
                    inverses[wide, LEAF:, :LEAF] = -lax.dot_general(
                        inv, part, (((1,), (0,)), ((), ())), precision=HIGHEST,
                        preferred_element_type=jnp.float32)
                if hi < total:
                    lower[hi:, lo:hi] = times_trans(lower[hi:, lo:hi], inv)
                    nxt = hi + LEAF
                    lower[hi:, hi:nxt] = lower[hi:, hi:nxt] - times_trans(
                        lower[hi:, :hi], lower[hi:nxt, :hi])

        return carry

    lax.fori_loop(0, n_leaf, step, 0)


def factor_head(first, second):
    width = first.shape[0]
    total = P_SIZE * width
    return pl.pallas_call(
        factor_kernel,
        out_shape=(
            jax.ShapeDtypeStruct((total, total), jnp.float32),
            jax.ShapeDtypeStruct((total // WIDE, WIDE, WIDE), jnp.float32),
        ),
        in_specs=[pl.BlockSpec(memory_space=pltpu.VMEM)] * 2,
        out_specs=(pl.BlockSpec(memory_space=pltpu.VMEM),) * 2,
        scratch_shapes=[
            pltpu.VMEM((LEAF, 2 * LEAF), jnp.float32),
            pltpu.VMEM((LEAF, LEAF), jnp.float32),
            pltpu.VMEM((LEAF, LEAF), jnp.float32),
        ],
        compiler_params=pltpu.CompilerParams(vmem_limit_bytes=32 << 20),
        cost_estimate=pl.CostEstimate(flops=10**10, bytes_accessed=10**7, transcendentals=0),
        name="factor_head",
    )(first, second)


def solve_into(out, lower, inverses):
    for wide in range(lower.shape[0] // WIDE):
        lo, hi = wide * WIDE, (wide + 1) * WIDE
        now = out[:, lo:hi]
        if wide:
            now = now - times_trans(out[:, :lo], lower[lo:hi, :lo])
        out[:, lo:hi] = times_trans(now, inverses[wide])


def own_kernel(live, panel, lower, inverses, factor):
    r = lax.axis_index("rows")
    width = panel.shape[0]

    @pl.when(r < P_SIZE)
    def _():
        factor[...] = lower[pl.ds(pl.multiple_of(lax.rem(r, P_SIZE) * width, width), width), :]

    @pl.when(r >= P_SIZE)
    def _():
        factor[...] = panel[...] * live[0]
        solve_into(factor, lower, inverses)


def own_rows(live, panel, lower, inverses):
    return pl.pallas_call(
        own_kernel,
        out_shape=jax.ShapeDtypeStruct(panel.shape, jnp.float32),
        in_specs=[pl.BlockSpec(memory_space=pltpu.SMEM)] + [pl.BlockSpec(memory_space=pltpu.VMEM)] * 3,
        out_specs=pl.BlockSpec(memory_space=pltpu.VMEM),
        compiler_params=pltpu.CompilerParams(vmem_limit_bytes=32 << 20),
        cost_estimate=pl.CostEstimate(flops=10**9, bytes_accessed=10**7, transcendentals=0),
        name="own_rows",
    )(live, panel, lower, inverses)


def update_kernel(target, lower, inverses, factor, window, updated, row):
    row[...] = target[...]
    solve_into(row, lower, inverses)
    updated[...] = window[...] - times_trans(factor[...], row[...])


def update_window(target, lower, inverses, factor, window):
    return pl.pallas_call(
        update_kernel,
        out_shape=jax.ShapeDtypeStruct(window.shape, jnp.float32),
        in_specs=[pl.BlockSpec(memory_space=pltpu.VMEM)] * 5,
        out_specs=pl.BlockSpec(memory_space=pltpu.VMEM),
        scratch_shapes=[pltpu.VMEM(target.shape, jnp.float32)],
        compiler_params=pltpu.CompilerParams(vmem_limit_bytes=40 << 20),
        cost_estimate=pl.CostEstimate(flops=10**9, bytes_accessed=10**7, transcendentals=0),
        name="update_window",
    )(target, lower, inverses, factor, window)


def shards(n_rows, n_cols, panel, window_block, row_live, window_rows):
    device_row = lax.axis_index("rows")
    device_col = lax.axis_index("cols")
    live = jnp.where(device_row < P_SIZE, 1, row_live[device_row]).astype(jnp.float32)
    first, second = spread(panel, n_rows, n_cols)
    first, second, panel = lax.optimization_barrier((first, second, panel))
    target = window_rows[device_col]
    kept = jnp.where(device_row == target, panel * live, 0)
    target_raw = lax.psum(kept, "rows")
    lower, inverses = factor_head(first, second)
    factor = own_rows(live[None], panel, lower, inverses)
    updated = update_window(target_raw, lower, inverses, factor, window_block)
    return (factor, updated)


def solution(mesh):
    in_specs = (P("rows", None), P("rows", "cols"), P(), P())
    out_specs = (P("rows", None), P("rows", "cols"))
    body = functools.partial(shards, mesh.shape["rows"], mesh.shape["cols"])
    return jax.shard_map(body, mesh=mesh, in_specs=in_specs, out_specs=out_specs, check_vma=False)
```

```python
import functools

import jax
import jax.numpy as jnp
from jax import lax
from jax.experimental import pallas as pl
from jax.experimental.pallas import tpu as pltpu
from jax.sharding import PartitionSpec as P

P_SIZE = 2
HIGHEST = lax.Precision.HIGHEST
CONTRACT = (((1,), (1,)), ((), ()))
PLAIN = (((1,), (0,)), ((), ()))
LEAF = 128
GROUP = 8
WIDE = 256
MESH = pl.DeviceIdType.MESH


def halves(value):
    high = value.astype(jnp.bfloat16)
    return high, (value - high.astype(jnp.float32)).astype(jnp.bfloat16)


def product(left, right, contract):
    lh, ll = halves(left)
    rh, rl = halves(right)

    def dot(a, b):
        return lax.dot_general(a, b, contract, preferred_element_type=jnp.float32)

    return dot(lh, rh) + (dot(lh, rl) + dot(ll, rh))


def times_trans(left, right):
    return product(left, right, CONTRACT)


def times(left, right):
    return product(left, right, PLAIN)


def spread_kernel(n_rows, panel, first, second, row_send, row_recv, far_send, far_recv, near_send, near_recv):
    r = lax.axis_index("rows")
    c = lax.axis_index("cols")
    far = lax.rem(c + 2, 4)
    near = c + 1 - 2 * lax.rem(c, 2)
    width = panel.shape[0]
    n_blocks = width // LEAF
    share = LEAF // 4
    pieces = [(which, b) for which in range(2) for b in range(n_blocks)]

    barrier = pltpu.get_barrier_semaphore()
    for other in (far, near):
        pl.semaphore_signal(barrier, inc=1, device_id=(r, other), device_id_type=MESH)

    @pl.when(r < 2)
    def _():
        pl.semaphore_signal(barrier, inc=1, device_id=(1 - r, c), device_id_type=MESH)

    @pl.when(r >= 2)
    def _():
        pl.semaphore_signal(barrier, inc=1, device_id=(r - 2, c), device_id_type=MESH)

    @pl.when(r + 2 < n_rows)
    def _():
        pl.semaphore_signal(barrier, inc=1, device_id=(r + 2, c), device_id_type=MESH)

    pl.semaphore_wait(barrier, 3 + (r + 2 < n_rows).astype(jnp.int32))

    def window(ref, piece, owner):
        which, b = pieces[piece]
        start = pl.multiple_of(b * LEAF + owner * share, 8)
        return ref.at[pl.ds(start, share), pl.ds(0, which * width + (b + 1) * LEAF)]

    def landing(piece, owner):
        return window((first, second)[pieces[piece][0]], piece, owner)

    def to_row(piece, slot, dest, own):
        return pltpu.make_async_remote_copy(
            src_ref=window(panel, piece, c) if own else landing(piece, c), dst_ref=landing(piece, c),
            send_sem=row_send.at[piece, slot], recv_sem=row_recv.at[piece],
            device_id=(dest, c), device_id_type=MESH)

    def to_far(piece):
        return pltpu.make_async_remote_copy(
            src_ref=landing(piece, c), dst_ref=landing(piece, c),
            send_sem=far_send.at[piece], recv_sem=far_recv.at[piece],
            device_id=(r, far), device_id_type=MESH)

    def to_near(piece, slot):
        owner = (c, far)[slot]
        return pltpu.make_async_remote_copy(
            src_ref=landing(piece, owner), dst_ref=landing(piece, owner),
            send_sem=near_send.at[piece, slot], recv_sem=near_recv.at[piece, slot],
            device_id=(r, near), device_id_type=MESH)

    for piece in range(len(pieces)):
        which = pieces[piece][0]

        @pl.when(r == which)
        def _():
            to_row(piece, 0, 1 - which, True).start()
            if which + 2 < n_rows:
                to_row(piece, 1, which + 2, True).start()

    @pl.when(r == 0)
    def _():
        first[...] = panel[:, :width]

    @pl.when(r == 1)
    def _():
        second[...] = panel[...]

    for piece in range(len(pieces) + 1):
        if piece < len(pieces):

            @pl.when(r != pieces[piece][0])
            def _():
                to_row(piece, 0, r, False).wait_recv()

                @pl.when(r + 2 < n_rows)
                def _():
                    to_row(piece, 0, r + 2, False).start()

                to_far(piece).start()
                to_near(piece, 0).start()

        if piece > 0:

            @pl.when(r != pieces[piece - 1][0])
            def _():
                to_far(piece - 1).wait_recv()
                to_near(piece - 1, 1).start()

    for piece in range(len(pieces)):
        which = pieces[piece][0]

        @pl.when(r != which)
        def _():
            for slot in range(2):
                to_near(piece, slot).wait_recv()
            for slot in range(2):
                to_near(piece, slot).wait_send()
            to_far(piece).wait_send()

            @pl.when(r + 2 < n_rows)
            def _():
                to_row(piece, 0, r + 2, False).wait_send()

        @pl.when(r == which)
        def _():
            to_row(piece, 0, 1 - which, True).wait_send()
            if which + 2 < n_rows:
                to_row(piece, 1, which + 2, True).wait_send()


def spread(panel, n_rows, n_cols):
    if n_cols != 4 or n_rows < 2:
        raise ValueError("unsupported mesh")
    width = panel.shape[0]
    n_pieces = 2 * (width // LEAF)
    return pl.pallas_call(
        functools.partial(spread_kernel, n_rows),
        out_shape=(
            jax.ShapeDtypeStruct((width, width), jnp.float32),
            jax.ShapeDtypeStruct((width, P_SIZE * width), jnp.float32),
        ),
        in_specs=[pl.BlockSpec(memory_space=pltpu.VMEM)],
        out_specs=(pl.BlockSpec(memory_space=pltpu.VMEM),) * 2,
        scratch_shapes=[
            pltpu.SemaphoreType.DMA((n_pieces, 2)),
            pltpu.SemaphoreType.DMA((n_pieces,)),
            pltpu.SemaphoreType.DMA((n_pieces,)),
            pltpu.SemaphoreType.DMA((n_pieces,)),
            pltpu.SemaphoreType.DMA((n_pieces, 2)),
            pltpu.SemaphoreType.DMA((n_pieces, 2)),
        ],
        compiler_params=pltpu.CompilerParams(
            collective_id=0, has_side_effects=True, vmem_limit_bytes=24 << 20),
        cost_estimate=pl.CostEstimate(flops=10**9, bytes_accessed=10**7, transcendentals=0),
        name="spread",
    )(panel)


def split3(value):
    high = value.astype(jnp.bfloat16).astype(jnp.float32)
    rest = value - high
    mid = rest.astype(jnp.bfloat16).astype(jnp.float32)
    return high, mid, rest - mid


def factor_leaf(aug, upper, inverse):
    lanes = lax.broadcasted_iota(jnp.int32, (GROUP, LEAF), 1)
    subs = lax.broadcasted_iota(jnp.int32, (GROUP, LEAF), 0)
    for g in range(LEAF // GROUP):
        base = g * GROUP
        left = aug[base : base + GROUP, :LEAF]
        right = aug[base : base + GROUP, LEAF:]
        cols = [
            jnp.broadcast_to(left[:, base + j : base + j + 1], (GROUP, LEAF)) for j in range(GROUP)
        ]
        scale = jnp.zeros((GROUP, LEAF), jnp.float32)
        for k in range(GROUP):
            pivot = jnp.broadcast_to(cols[k][k : k + 1, :], (GROUP, LEAF))
            root = lax.rsqrt(pivot)
            scale = jnp.where(subs == k, root, scale)
            if k + 1 < GROUP:
                mult = jnp.where(subs > k, cols[k] * (root * root), 0.0)
                for j in range(k + 1, GROUP):
                    cols[j] = cols[j] - mult * jnp.broadcast_to(cols[j][k : k + 1, :], (GROUP, LEAF))
                left = left - mult * jnp.broadcast_to(left[k : k + 1, :], (GROUP, LEAF))
                right = right - mult * jnp.broadcast_to(right[k : k + 1, :], (GROUP, LEAF))
        row_of = lanes - base
        left = jnp.where(row_of >= subs, left * scale, 0.0)
        right = right * scale
        upper[base : base + GROUP, :] = left
        inverse[base : base + GROUP, :] = right
        if base + GROUP < LEAF:
            lh, lm, ll = split3(left)
            rh, rm, rl = split3(right)
            keep = lanes >= base + GROUP
            a = [jnp.where(keep, v, 0.0) for v in (lh, lm, ll)]
            lhs = jnp.concatenate([a[0], a[0], a[1], a[0], a[1], a[2]], axis=0)
            rl_ = jnp.concatenate([lh, lm, lh, ll, lm, lh], axis=0)
            rr_ = jnp.concatenate([rh, rm, rh, rl, rm, rh], axis=0)
            rhs = jnp.concatenate([rl_, rr_], axis=1)
            update = lax.dot_general(
                lhs, rhs, (((0,), (0,)), ((), ())), preferred_element_type=jnp.float32)
            aug[base + GROUP :, :] = aug[base + GROUP :, :] - update[base + GROUP :, :]


def factor_kernel(live, first, second, panel, factor, solved, lower, inverses, aug, upper, leaf_inv):
    width = first.shape[0]
    total = lower.shape[0]
    n_leaf = total // LEAF
    per = width // LEAF
    rows = lax.broadcasted_iota(jnp.int32, (LEAF, LEAF), 0)
    lanes = lax.broadcasted_iota(jnp.int32, (LEAF, LEAF), 1)
    lower[:width, :width] = first[...]
    lower[:width, width:] = jnp.zeros((width, total - width), jnp.float32)
    lower[width:, :] = second[...]
    for b in range(n_leaf - 1):
        lower[b * LEAF : (b + 1) * LEAF, (b + 1) * LEAF :] = jnp.zeros(
            (LEAF, total - (b + 1) * LEAF), jnp.float32)
    inverses[...] = jnp.zeros(inverses.shape, jnp.float32)

    def step(k, carry):
        at = pl.ds(pl.multiple_of(k * LEAF, LEAF), LEAF)
        block = lower[at, at]
        aug[:, :LEAF] = jnp.where(rows >= lanes, block, block.T)
        aug[:, LEAF:] = jnp.where(rows == lanes, 1.0, 0.0)
        factor_leaf(aug, upper, leaf_inv)
        lower[at, at] = upper[...].T
        for b in range(n_leaf):

            @pl.when(k == b)
            def _():
                lo, hi = b * LEAF, (b + 1) * LEAF
                wide = b * LEAF // WIDE
                off = lo - wide * WIDE
                inv = leaf_inv[...]
                inverses[wide, off : off + LEAF, off : off + LEAF] = inv
                if off:
                    before = inverses[wide, :LEAF, :LEAF]
                    cross = lower[lo:hi, lo - LEAF : lo]
                    part = lax.dot_general(
                        cross, before, (((1,), (0,)), ((), ())), precision=HIGHEST,
                        preferred_element_type=jnp.float32)
                    inverses[wide, LEAF:, :LEAF] = -lax.dot_general(
                        inv, part, (((1,), (0,)), ((), ())), precision=HIGHEST,
                        preferred_element_type=jnp.float32)
                if hi < total:
                    lower[hi:, lo:hi] = times_trans(lower[hi:, lo:hi], inv)
                    nxt = hi + LEAF
                    lower[hi:, hi:nxt] = lower[hi:, hi:nxt] - times_trans(
                        lower[hi:, :hi], lower[hi:nxt, :hi])

        return carry

    lax.fori_loop(0, n_leaf, step, 0)

    r = lax.axis_index("rows")
    n_wide = total // WIDE

    @pl.when(r < P_SIZE)
    def _():
        factor[...] = lower[pl.ds(pl.multiple_of(lax.rem(r, P_SIZE) * width, width), width), :]

    @pl.when(r >= P_SIZE)
    def _():
        factor[...] = panel[...] * live[0]
        for wide in range(n_wide):
            lo, hi = wide * WIDE, (wide + 1) * WIDE
            now = factor[:, lo:hi]
            if wide:
                now = now - times_trans(factor[:, :lo], lower[lo:hi, :lo])
            factor[:, lo:hi] = times_trans(now, inverses[wide])

    for wide in reversed(range(n_wide)):
        lo, hi = wide * WIDE, (wide + 1) * WIDE
        now = factor[:, lo:hi]
        if hi < total:
            now = now - times(solved[:, hi:], lower[hi:, lo:hi])
        solved[:, lo:hi] = times(now, inverses[wide])


def factor_rows(live, first, second, panel):
    width = first.shape[0]
    total = P_SIZE * width
    return pl.pallas_call(
        factor_kernel,
        out_shape=(jax.ShapeDtypeStruct(panel.shape, jnp.float32),) * 2,
        in_specs=[pl.BlockSpec(memory_space=pltpu.SMEM)] + [pl.BlockSpec(memory_space=pltpu.VMEM)] * 3,
        out_specs=(pl.BlockSpec(memory_space=pltpu.VMEM),) * 2,
        scratch_shapes=[
            pltpu.VMEM((total, total), jnp.float32),
            pltpu.VMEM((total // WIDE, WIDE, WIDE), jnp.float32),
            pltpu.VMEM((LEAF, 2 * LEAF), jnp.float32),
            pltpu.VMEM((LEAF, LEAF), jnp.float32),
            pltpu.VMEM((LEAF, LEAF), jnp.float32),
        ],
        compiler_params=pltpu.CompilerParams(vmem_limit_bytes=40 << 20),
        cost_estimate=pl.CostEstimate(flops=10**10, bytes_accessed=10**7, transcendentals=0),
        name="factor_rows",
    )(live, first, second, panel)


def update_kernel(solved, target, window, updated):
    updated[...] = window[...] - times_trans(solved[...], target[...])


def update_window(solved, target, window):
    return pl.pallas_call(
        update_kernel,
        out_shape=jax.ShapeDtypeStruct(window.shape, jnp.float32),
        in_specs=[pl.BlockSpec(memory_space=pltpu.VMEM)] * 3,
        out_specs=pl.BlockSpec(memory_space=pltpu.VMEM),
        compiler_params=pltpu.CompilerParams(vmem_limit_bytes=40 << 20),
        cost_estimate=pl.CostEstimate(flops=10**9, bytes_accessed=10**7, transcendentals=0),
        name="update_window",
    )(solved, target, window)


def shards(n_rows, n_cols, panel, window_block, row_live, window_rows):
    device_row = lax.axis_index("rows")
    device_col = lax.axis_index("cols")
    live = jnp.where(device_row < P_SIZE, 1, row_live[device_row]).astype(jnp.float32)
    target = window_rows[device_col]
    kept = jnp.where(device_row == target, panel * live, 0)
    kept, panel = lax.optimization_barrier((kept, panel))
    target_raw = lax.psum(kept, "rows")
    first, second = spread(panel, n_rows, n_cols)
    factor, solved = factor_rows(live[None], first, second, panel)
    updated = update_window(solved, target_raw, window_block)
    return (factor, updated)


def solution(mesh):
    in_specs = (P("rows", None), P("rows", "cols"), P(), P())
    out_specs = (P("rows", None), P("rows", "cols"))
    body = functools.partial(shards, mesh.shape["rows"], mesh.shape["cols"])
    return jax.shard_map(body, mesh=mesh, in_specs=in_specs, out_specs=out_specs, check_vma=False)
```

```python
import functools

import jax
import jax.numpy as jnp
from jax import lax
from jax.experimental import pallas as pl
from jax.experimental.pallas import tpu as pltpu
from jax.sharding import PartitionSpec as P

P_SIZE = 2
HIGHEST = lax.Precision.HIGHEST
CONTRACT = (((1,), (1,)), ((), ()))
PLAIN = (((1,), (0,)), ((), ()))
LEAF = 128
GROUP = 16
WIDE = 256
MESH = pl.DeviceIdType.MESH


def halves(value):
    high = value.astype(jnp.bfloat16)
    return high, (value - high.astype(jnp.float32)).astype(jnp.bfloat16)


def product(left, right, contract):
    lh, ll = halves(left)
    rh, rl = halves(right)

    def dot(a, b):
        return lax.dot_general(a, b, contract, preferred_element_type=jnp.float32)

    return dot(lh, rh) + (dot(lh, rl) + dot(ll, rh))


def times_trans(left, right):
    return product(left, right, CONTRACT)


def times(left, right):
    return product(left, right, PLAIN)


def spread_kernel(n_rows, panel, first, second, row_send, row_recv, far_send, far_recv, near_send, near_recv):
    r = lax.axis_index("rows")
    c = lax.axis_index("cols")
    far = lax.rem(c + 2, 4)
    near = c + 1 - 2 * lax.rem(c, 2)
    width = panel.shape[0]
    n_blocks = width // LEAF
    share = LEAF // 4
    pieces = [(which, b) for which in range(2) for b in range(n_blocks)]

    barrier = pltpu.get_barrier_semaphore()
    for other in (far, near):
        pl.semaphore_signal(barrier, inc=1, device_id=(r, other), device_id_type=MESH)

    @pl.when(r < 2)
    def _():
        pl.semaphore_signal(barrier, inc=1, device_id=(1 - r, c), device_id_type=MESH)

    @pl.when(r >= 2)
    def _():
        pl.semaphore_signal(barrier, inc=1, device_id=(r - 2, c), device_id_type=MESH)

    @pl.when(r + 2 < n_rows)
    def _():
        pl.semaphore_signal(barrier, inc=1, device_id=(r + 2, c), device_id_type=MESH)

    pl.semaphore_wait(barrier, 3 + (r + 2 < n_rows).astype(jnp.int32))

    def window(ref, piece, owner):
        which, b = pieces[piece]
        start = pl.multiple_of(b * LEAF + owner * share, 8)
        return ref.at[pl.ds(start, share), pl.ds(0, which * width + (b + 1) * LEAF)]

    def landing(piece, owner):
        return window((first, second)[pieces[piece][0]], piece, owner)

    def to_row(piece, slot, dest, own):
        return pltpu.make_async_remote_copy(
            src_ref=window(panel, piece, c) if own else landing(piece, c), dst_ref=landing(piece, c),
            send_sem=row_send.at[piece, slot], recv_sem=row_recv.at[piece],
            device_id=(dest, c), device_id_type=MESH)

    def to_far(piece):
        return pltpu.make_async_remote_copy(
            src_ref=landing(piece, c), dst_ref=landing(piece, c),
            send_sem=far_send.at[piece], recv_sem=far_recv.at[piece],
            device_id=(r, far), device_id_type=MESH)

    def to_near(piece, slot):
        owner = (c, far)[slot]
        return pltpu.make_async_remote_copy(
            src_ref=landing(piece, owner), dst_ref=landing(piece, owner),
            send_sem=near_send.at[piece, slot], recv_sem=near_recv.at[piece, slot],
            device_id=(r, near), device_id_type=MESH)

    for piece in range(len(pieces)):
        which = pieces[piece][0]

        @pl.when(r == which)
        def _():
            to_row(piece, 0, 1 - which, True).start()
            if which + 2 < n_rows:
                to_row(piece, 1, which + 2, True).start()

    @pl.when(r == 0)
    def _():
        first[...] = panel[:, :width]

    @pl.when(r == 1)
    def _():
        second[...] = panel[...]

    for piece in range(len(pieces) + 1):
        if piece < len(pieces):

            @pl.when(r != pieces[piece][0])
            def _():
                to_row(piece, 0, r, False).wait_recv()

                @pl.when(r + 2 < n_rows)
                def _():
                    to_row(piece, 0, r + 2, False).start()

                to_far(piece).start()
                to_near(piece, 0).start()

        if piece > 0:

            @pl.when(r != pieces[piece - 1][0])
            def _():
                to_far(piece - 1).wait_recv()
                to_near(piece - 1, 1).start()

    for piece in range(len(pieces)):
        which = pieces[piece][0]

        @pl.when(r != which)
        def _():
            for slot in range(2):
                to_near(piece, slot).wait_recv()
            for slot in range(2):
                to_near(piece, slot).wait_send()
            to_far(piece).wait_send()

            @pl.when(r + 2 < n_rows)
            def _():
                to_row(piece, 0, r + 2, False).wait_send()

        @pl.when(r == which)
        def _():
            to_row(piece, 0, 1 - which, True).wait_send()
            if which + 2 < n_rows:
                to_row(piece, 1, which + 2, True).wait_send()


def spread(panel, n_rows, n_cols):
    if n_cols != 4 or n_rows < 2:
        raise ValueError("unsupported mesh")
    width = panel.shape[0]
    n_pieces = 2 * (width // LEAF)
    return pl.pallas_call(
        functools.partial(spread_kernel, n_rows),
        out_shape=(
            jax.ShapeDtypeStruct((width, width), jnp.float32),
            jax.ShapeDtypeStruct((width, P_SIZE * width), jnp.float32),
        ),
        in_specs=[pl.BlockSpec(memory_space=pltpu.VMEM)],
        out_specs=(pl.BlockSpec(memory_space=pltpu.VMEM),) * 2,
        scratch_shapes=[
            pltpu.SemaphoreType.DMA((n_pieces, 2)),
            pltpu.SemaphoreType.DMA((n_pieces,)),
            pltpu.SemaphoreType.DMA((n_pieces,)),
            pltpu.SemaphoreType.DMA((n_pieces,)),
            pltpu.SemaphoreType.DMA((n_pieces, 2)),
            pltpu.SemaphoreType.DMA((n_pieces, 2)),
        ],
        compiler_params=pltpu.CompilerParams(
            collective_id=0, has_side_effects=True, vmem_limit_bytes=24 << 20),
        cost_estimate=pl.CostEstimate(flops=10**9, bytes_accessed=10**7, transcendentals=0),
        name="spread",
    )(panel)


def split3(value):
    high = value.astype(jnp.bfloat16).astype(jnp.float32)
    rest = value - high
    mid = rest.astype(jnp.bfloat16).astype(jnp.float32)
    return high, mid, rest - mid


def factor_leaf(aug, upper, inverse):
    lanes = lax.broadcasted_iota(jnp.int32, (GROUP, LEAF), 1)
    subs = lax.broadcasted_iota(jnp.int32, (GROUP, LEAF), 0)
    for g in range(LEAF // GROUP):
        base = g * GROUP
        left = aug[base : base + GROUP, :LEAF]
        right = aug[base : base + GROUP, LEAF:]
        cols = [
            jnp.broadcast_to(left[:, base + j : base + j + 1], (GROUP, LEAF)) for j in range(GROUP)
        ]
        scale = jnp.zeros((GROUP, LEAF), jnp.float32)
        for k in range(GROUP):
            pivot = jnp.broadcast_to(cols[k][k : k + 1, :], (GROUP, LEAF))
            root = lax.rsqrt(pivot)
            scale = jnp.where(subs == k, root, scale)
            if k + 1 < GROUP:
                mult = jnp.where(subs > k, cols[k] * (root * root), 0.0)
                for j in range(k + 1, GROUP):
                    cols[j] = cols[j] - mult * jnp.broadcast_to(cols[j][k : k + 1, :], (GROUP, LEAF))
                left = left - mult * jnp.broadcast_to(left[k : k + 1, :], (GROUP, LEAF))
                right = right - mult * jnp.broadcast_to(right[k : k + 1, :], (GROUP, LEAF))
        row_of = lanes - base
        left = jnp.where(row_of >= subs, left * scale, 0.0)
        right = right * scale
        upper[base : base + GROUP, :] = left
        inverse[base : base + GROUP, :] = right
        if base + GROUP < LEAF:
            lh, lm, ll = split3(left)
            rh, rm, rl = split3(right)
            keep = lanes >= base + GROUP
            a = [jnp.where(keep, v, 0.0) for v in (lh, lm, ll)]
            lhs = jnp.concatenate([a[0], a[0], a[1], a[0], a[1], a[2]], axis=0)
            rl_ = jnp.concatenate([lh, lm, lh, ll, lm, lh], axis=0)
            rr_ = jnp.concatenate([rh, rm, rh, rl, rm, rh], axis=0)
            rhs = jnp.concatenate([rl_, rr_], axis=1)
            update = lax.dot_general(
                lhs, rhs, (((0,), (0,)), ((), ())), preferred_element_type=jnp.float32)
            aug[base + GROUP :, :] = aug[base + GROUP :, :] - update[base + GROUP :, :]


def factor_kernel(live, first, second, panel, factor, solved, lower, inverses, aug, upper, leaf_inv):
    width = first.shape[0]
    total = lower.shape[0]
    n_leaf = total // LEAF
    per = width // LEAF
    rows = lax.broadcasted_iota(jnp.int32, (LEAF, LEAF), 0)
    lanes = lax.broadcasted_iota(jnp.int32, (LEAF, LEAF), 1)
    lower[:width, :width] = first[...]
    lower[:width, width:] = jnp.zeros((width, total - width), jnp.float32)
    lower[width:, :] = second[...]
    for b in range(n_leaf - 1):
        lower[b * LEAF : (b + 1) * LEAF, (b + 1) * LEAF :] = jnp.zeros(
            (LEAF, total - (b + 1) * LEAF), jnp.float32)
    inverses[...] = jnp.zeros(inverses.shape, jnp.float32)

    def step(k, carry):
        at = pl.ds(pl.multiple_of(k * LEAF, LEAF), LEAF)
        block = lower[at, at]
        aug[:, :LEAF] = jnp.where(rows >= lanes, block, block.T)
        aug[:, LEAF:] = jnp.where(rows == lanes, 1.0, 0.0)
        factor_leaf(aug, upper, leaf_inv)
        lower[at, at] = upper[...].T
        for b in range(n_leaf):

            @pl.when(k == b)
            def _():
                lo, hi = b * LEAF, (b + 1) * LEAF
                wide = b * LEAF // WIDE
                off = lo - wide * WIDE
                inv = leaf_inv[...]
                inverses[wide, off : off + LEAF, off : off + LEAF] = inv
                if off:
                    before = inverses[wide, :LEAF, :LEAF]
                    cross = lower[lo:hi, lo - LEAF : lo]
                    part = lax.dot_general(
                        cross, before, (((1,), (0,)), ((), ())), precision=HIGHEST,
                        preferred_element_type=jnp.float32)
                    inverses[wide, LEAF:, :LEAF] = -lax.dot_general(
                        inv, part, (((1,), (0,)), ((), ())), precision=HIGHEST,
                        preferred_element_type=jnp.float32)
                if hi < total:
                    lower[hi:, lo:hi] = times_trans(lower[hi:, lo:hi], inv)
                    nxt = hi + LEAF
                    lower[hi:, hi:nxt] = lower[hi:, hi:nxt] - times_trans(
                        lower[hi:, :hi], lower[hi:nxt, :hi])

        return carry

    lax.fori_loop(0, n_leaf, step, 0)

    r = lax.axis_index("rows")
    n_wide = total // WIDE

    @pl.when(r < P_SIZE)
    def _():
        factor[...] = lower[pl.ds(pl.multiple_of(lax.rem(r, P_SIZE) * width, width), width), :]

    @pl.when(r >= P_SIZE)
    def _():
        factor[...] = panel[...] * live[0]
        for wide in range(n_wide):
            lo, hi = wide * WIDE, (wide + 1) * WIDE
            now = factor[:, lo:hi]
            if wide:
                now = now - times_trans(factor[:, :lo], lower[lo:hi, :lo])
            factor[:, lo:hi] = times_trans(now, inverses[wide])

    for wide in reversed(range(n_wide)):
        lo, hi = wide * WIDE, (wide + 1) * WIDE
        now = factor[:, lo:hi]
        if hi < total:
            now = now - times(solved[:, hi:], lower[hi:, lo:hi])
        solved[:, lo:hi] = times(now, inverses[wide])


def factor_rows(live, first, second, panel):
    width = first.shape[0]
    total = P_SIZE * width
    return pl.pallas_call(
        factor_kernel,
        out_shape=(jax.ShapeDtypeStruct(panel.shape, jnp.float32),) * 2,
        in_specs=[pl.BlockSpec(memory_space=pltpu.SMEM)] + [pl.BlockSpec(memory_space=pltpu.VMEM)] * 3,
        out_specs=(pl.BlockSpec(memory_space=pltpu.VMEM),) * 2,
        scratch_shapes=[
            pltpu.VMEM((total, total), jnp.float32),
            pltpu.VMEM((total // WIDE, WIDE, WIDE), jnp.float32),
            pltpu.VMEM((LEAF, 2 * LEAF), jnp.float32),
            pltpu.VMEM((LEAF, LEAF), jnp.float32),
            pltpu.VMEM((LEAF, LEAF), jnp.float32),
        ],
        compiler_params=pltpu.CompilerParams(vmem_limit_bytes=40 << 20),
        cost_estimate=pl.CostEstimate(flops=10**10, bytes_accessed=10**7, transcendentals=0),
        name="factor_rows",
    )(live, first, second, panel)


def update_kernel(solved, target, window, updated):
    updated[...] = window[...] - times_trans(solved[...], target[...])


def update_window(solved, target, window):
    return pl.pallas_call(
        update_kernel,
        out_shape=jax.ShapeDtypeStruct(window.shape, jnp.float32),
        in_specs=[pl.BlockSpec(memory_space=pltpu.VMEM)] * 3,
        out_specs=pl.BlockSpec(memory_space=pltpu.VMEM),
        compiler_params=pltpu.CompilerParams(vmem_limit_bytes=40 << 20),
        cost_estimate=pl.CostEstimate(flops=10**9, bytes_accessed=10**7, transcendentals=0),
        name="update_window",
    )(solved, target, window)


def shards(n_rows, n_cols, panel, window_block, row_live, window_rows):
    device_row = lax.axis_index("rows")
    device_col = lax.axis_index("cols")
    live = jnp.where(device_row < P_SIZE, 1, row_live[device_row]).astype(jnp.float32)
    target = window_rows[device_col]
    kept = jnp.where(device_row == target, panel * live, 0)
    kept, panel = lax.optimization_barrier((kept, panel))
    target_raw = lax.psum(kept, "rows")
    first, second = spread(panel, n_rows, n_cols)
    factor, solved = factor_rows(live[None], first, second, panel)
    updated = update_window(solved, target_raw, window_block)
    return (factor, updated)


def solution(mesh):
    in_specs = (P("rows", None), P("rows", "cols"), P(), P())
    out_specs = (P("rows", None), P("rows", "cols"))
    body = functools.partial(shards, mesh.shape["rows"], mesh.shape["cols"])
    return jax.shard_map(body, mesh=mesh, in_specs=in_specs, out_specs=out_specs, check_vma=False)
```
